32 devices in a mesh: seq: 16 (over z, x, core), head: 2 (over y).
Axes of the slice: x: 2, y: 2, z: 4, core: 2. Of those that a mesh axis runs over, the one named last changes fastest.
Arguments:
- tokens: bfloat16 [8192, 1024], P('seq'), may hold values from -6 to 6
- mem_query_w: bfloat16 [1024, 1024], P(None, 'head'), may hold values from -0.1875 to 0.1875
- mem_key_w: bfloat16 [1024, 1024], P(None, 'head'), may hold values from -0.1875 to 0.1875
- mem_value_w: bfloat16 [1024, 1024], P(None, 'head'), may hold values from -0.1875 to 0.1875
- mem_in: float32 [1024, 1024], P(None, 'head'), may hold values from -0.1875 to 0.1875
- mem_out: float32 [1024, 1024], P('head'), may hold values from -0.1875 to 0.1875
- forget_levels: float32 [16, 1024], P(None, 'head'), may hold values from 0.003 to 0.3
- momentum_levels: float32 [16, 1024], P(None, 'head'), may hold values from 0.2 to 0.9
- step_levels: float32 [16, 1024], P(None, 'head'), may hold values from 0.02 to 0.2
- plan: int32 [16], P('seq'), may hold values from 0 to 15
- norm_gain: float32 [1024], replicated, may hold values from 0.5 to 1.5
- attn_query_w: bfloat16 [1024, 1024], P(None, 'head'), may hold values from -1 to 1
- attn_key_w: bfloat16 [1024, 1024], P(None, 'head'), may hold values from -4 to 4
- attn_value_w: bfloat16 [1024, 1024], P(None, 'head'), may hold values from -0.1875 to 0.1875
- attn_out_w: bfloat16 [1024, 1024], P('head'), may hold values from -0.25 to 0.25
Outputs:
- layer_out: bfloat16 [8192, 1024], P('seq', 'head')
The draws below stay inside these ranges and needn't reach their ends.
All inputs are finite; a program needn't handle non-finite values.
Results may differ from the reference program's by a relative error of at most 0.014.
Values may be sent and summed in bfloat16 or wider, within the bound.
A program may use at most 192 MiB of HBM per device.

```python
import math
import jax
import jax.numpy as jnp
from jax import lax

D = 1024
HEAD_DIM = 64
MEM_HID = 1024
LEVELS = 16
SPAN = 8
TOK_DEV = 512
GROUPS = 16
LENGTH = 8192


def attention_pair(key):
    shared = jax.random.normal(jax.random.fold_in(key, 11), (D, D), jnp.float32) / math.sqrt(D)
    others = jax.random.normal(jax.random.fold_in(key, 12), (D, D), jnp.float32) / math.sqrt(D)
    return (shared, others)


def draw_attn_query_w(key, part):
    shared, others = attention_pair(key)
    return jnp.clip(shared, -1.0, 1.0).astype(jnp.bfloat16)


def draw_attn_key_w(key, part):
    shared, others = attention_pair(key)
    return jnp.clip(others, -4.0, 4.0).astype(jnp.bfloat16)


def touch_ends(array, key, smallest, largest):
    extent = array.shape
    spot = [jax.random.randint(jax.random.fold_in(key, axis), (), 0, extent[axis]) for axis in range(len(extent))]
    array = array.at[tuple(spot)].set(smallest)
    longest = extent.index(max(extent))
    spot[longest] = (spot[longest] + 1) % extent[longest]
    return array.at[tuple(spot)].set(largest)


def spiked(drawn, stream_key, source, target, shards_of, factor):
    def block_of(position):
        return (jnp.arange(drawn.shape[position]) // (drawn.shape[position] // shards_of)).reshape((-1,) + (1,) * (drawn.ndim - 1 - position))

    near = jax.random.permutation(stream_key, shards_of)[block_of(target)]
    far = (block_of(target) + shards_of // 2) % shards_of
    return jnp.where((block_of(source) == near) | (block_of(source) == far), factor * drawn, drawn)


def shard_levels(own_key, extent, split, least, largest):
    factor_of = 1.0
    for position, shards_of in split:
        steps = jax.random.uniform(jax.random.fold_in(jax.random.fold_in(own_key, 6), position), (shards_of,), jnp.float32, least / len(split), largest / len(split))
        factor_of = factor_of * jnp.repeat(jnp.exp(steps), extent[position] // shards_of).reshape((-1,) + (1,) * (len(extent) - 1 - position))
    return factor_of


def scatter_about(rng, extent, spread, most, split=(), kind=jnp.bfloat16):
    factor_of = shard_levels(rng, extent, split, -0.22, 0.18) if split else 1.0
    result = jax.random.normal(rng, extent, jnp.float32) * spread * factor_of
    return jnp.minimum(jnp.maximum(result, -most), most).astype(kind)


def heavy_noise(own_key, dims, width, limit, shards, heavy, kind=jnp.bfloat16):
    result = width * jax.random.normal(own_key, dims, jnp.float32)
    if shards:
        result = result * shard_levels(own_key, dims, shards, -0.22, 0.18)
    return jnp.clip(spiked(result, jax.random.fold_in(own_key, 3), *heavy), -limit, limit).astype(kind)


def setup_inputs(seed: int = 0) -> dict:
    splits = jax.random.split(jax.random.key(seed), 16)
    tokens = scatter_about(splits[0], (LENGTH, D), 1.0, 6.0, ((0, 16),))
    mem_query_w = scatter_about(splits[1], (D, D), D ** -0.5, 0.1875, ((1, 2),))
    mem_key_w = scatter_about(splits[2], (D, D), D ** -0.5, 0.1875, ((1, 2),))
    mem_value_w = scatter_about(splits[3], (D, D), D ** -0.5, 0.1875, ((1, 2),))
    mem_in = scatter_about(splits[4], (D, MEM_HID), D ** -0.5, 0.1875, ((1, 2),), jnp.float32)
    mem_out = scatter_about(splits[5], (MEM_HID, D), MEM_HID ** -0.5, 0.1875, ((0, 2),), jnp.float32)
    forget_levels = jnp.clip(jnp.exp(math.log(0.3) - 4.6051702 * jax.random.uniform(splits[6], (LEVELS, MEM_HID), jnp.float32) ** shard_levels(splits[6], (LEVELS, MEM_HID), ((1, 2),), -0.2, 0.2)), 0.003, 0.3)
    momentum_levels = jnp.clip(0.2 + 0.7 * jax.random.uniform(splits[7], (LEVELS, MEM_HID), jnp.float32) ** shard_levels(splits[7], (LEVELS, MEM_HID), ((1, 2),), -0.2, 0.2), 0.2, 0.9)
    step_levels = jnp.clip(jnp.exp(math.log(0.2) - 2.3025851 * jax.random.uniform(splits[8], (LEVELS, MEM_HID), jnp.float32) ** shard_levels(splits[8], (LEVELS, MEM_HID), ((1, 2),), -0.2, 0.2)), 0.02, 0.2)
    plan = touch_ends(jax.random.randint(splits[9], (GROUPS,), 0, LEVELS), jax.random.fold_in(splits[9], 1), 0, LEVELS - 1).astype(jnp.int32)
    norm_gain = jnp.clip(1.0 + 0.1 * jax.random.normal(splits[10], (D,), jnp.float32), 0.5, 1.5)
    attn_query_w = draw_attn_query_w(jax.random.fold_in(splits[15], 71), 0)
    attn_key_w = draw_attn_key_w(jax.random.fold_in(splits[15], 71), 0)
    attn_value_w = scatter_about(splits[13], (D, D), D ** -0.5, 0.1875, ((1, 2),))
    attn_out_w = heavy_noise(splits[14], (D, D), D ** -0.5, 0.25, ((0, 2),), (0, 1, 2, 2.0))
    return {"tokens": tokens, "mem_query_w": mem_query_w, "mem_key_w": mem_key_w, "mem_value_w": mem_value_w, "mem_in": mem_in, "mem_out": mem_out, "forget_levels": forget_levels, "momentum_levels": momentum_levels, "step_levels": step_levels, "plan": plan, "norm_gain": norm_gain, "attn_query_w": attn_query_w, "attn_key_w": attn_key_w, "attn_value_w": attn_value_w, "attn_out_w": attn_out_w}


highest = lax.Precision.HIGHEST
epsilon = 1e-06

def silu_slope(values):
    sigmoid = jax.nn.sigmoid(values)
    return sigmoid * (1.0 + values * (1.0 - sigmoid))

def project(left, weight):
    return jnp.dot(left, weight, preferred_element_type=jnp.float32).astype(jnp.bfloat16)

def normalize(retrieved, norm_gain):
    mean_square = lax.optimization_barrier(jnp.mean(retrieved * retrieved, axis=-1, keepdims=True))
    return (retrieved * lax.rsqrt(mean_square + epsilon) * norm_gain).astype(jnp.bfloat16)

def window_attend(query, keys, values, block_index, head_dim):
    query_count = query.shape[0]
    key_count = keys.shape[0]
    head_count = query.shape[1] // head_dim
    query_heads = query.reshape(query_count, head_count, head_dim).astype(jnp.float32)
    key_heads = keys.reshape(key_count, head_count, head_dim).astype(jnp.float32)
    value_heads = values.reshape(key_count, head_count, head_dim).astype(jnp.float32)
    scores = jnp.einsum('qhd,khd->hqk', query_heads, key_heads) * head_dim ** (-0.5)
    span_rows = key_count - query_count
    distance = span_rows + jnp.arange(query_count, dtype=jnp.int32)[:, None] - jnp.arange(key_count, dtype=jnp.int32)[None, :]
    key_pos = (block_index * query_count - span_rows + jnp.arange(key_count, dtype=jnp.int32))[None, :]
    allowed = (distance >= 0) & (distance < span_rows) & (key_pos >= 0)
    scores = jnp.where(allowed[None], scores, -1e+30)
    row_peak = lax.optimization_barrier(jnp.max(scores, axis=-1, keepdims=True))
    weights = jnp.exp(scores - row_peak)
    probabilities = (weights / lax.optimization_barrier(jnp.sum(weights, axis=-1, keepdims=True))).astype(jnp.bfloat16)
    context = jnp.einsum('hqk,khd->qhd', probabilities.astype(jnp.float32), value_heads)
    return context.reshape(query_count, head_count * head_dim).astype(jnp.bfloat16)

def reference(tokens, mem_query_w, mem_key_w, mem_value_w, mem_in, mem_out, forget_levels, momentum_levels, step_levels, plan, norm_gain, attn_query_w, attn_key_w, attn_value_w, attn_out_w):
    mem_query = project(tokens, mem_query_w).reshape(GROUPS, TOK_DEV, D)
    mem_key = project(tokens, mem_key_w).reshape(GROUPS, TOK_DEV, D)
    mem_value = project(tokens, mem_value_w).reshape(GROUPS, TOK_DEV, D)

    def group_step(state_now, inputs):
        speed_in, speed_out, weight_in, weight_out = state_now
        query_rows, key_rows, value_rows, chosen = inputs
        keys_wide = key_rows.astype(jnp.float32)
        pre_act = jnp.dot(keys_wide, mem_in, precision=highest)
        hidden = jax.nn.silu(pre_act)
        predicted = jnp.dot(hidden, mem_out, precision=highest)
        residual_err = 2.0 / TOK_DEV * (predicted - value_rows.astype(jnp.float32))
        grad_out = jnp.dot(hidden.T, residual_err, precision=highest)
        slope_term = jnp.dot(residual_err, mem_out.T, precision=highest) * silu_slope(pre_act)
        grad_in = jnp.dot(keys_wide.T, slope_term, precision=highest)
        query_wide = query_rows.astype(jnp.float32)
        retrieved = jnp.dot(jax.nn.silu(jnp.dot(query_wide, weight_in, precision=highest)), weight_out, precision=highest)
        forget = forget_levels[chosen]
        momentum = momentum_levels[chosen]
        step_rate = step_levels[chosen]
        speed_in = momentum[None, :] * speed_in - step_rate[None, :] * grad_in
        speed_out = momentum[:, None] * speed_out - step_rate[:, None] * grad_out
        weight_in = (1.0 - forget)[None, :] * weight_in + speed_in
        weight_out = (1.0 - forget)[:, None] * weight_out + speed_out
        return ((speed_in, speed_out, weight_in, weight_out), retrieved)
    initial = (jnp.zeros_like(mem_in), jnp.zeros_like(mem_out), mem_in, mem_out)
    last_state, retrieved = lax.scan(group_step, initial, (mem_query, mem_key, mem_value, plan))
    normed = normalize(retrieved.reshape(LENGTH, D), norm_gain)
    att_query = project(normed, attn_query_w)
    att_key = project(normed, attn_key_w)
    att_value = project(normed, attn_value_w)
    span_rows = SPAN * TOK_DEV
    padding = jnp.zeros((span_rows, D), jnp.bfloat16)
    key_padded = jnp.concatenate([padding, att_key], axis=0)
    value_padded = jnp.concatenate([padding, att_value], axis=0)

    def attend_block(block_index):
        begin = block_index * TOK_DEV
        query_block = lax.dynamic_slice_in_dim(att_query, begin, TOK_DEV, 0)
        key_block = lax.dynamic_slice_in_dim(key_padded, begin, span_rows + TOK_DEV, 0)
        value_block = lax.dynamic_slice_in_dim(value_padded, begin, span_rows + TOK_DEV, 0)
        return window_attend(query_block, key_block, value_block, block_index, HEAD_DIM)
    context = lax.map(attend_block, jnp.arange(GROUPS, dtype=jnp.int32)).reshape(LENGTH, D)
    return project(context, attn_out_w)
```

```python
import functools
import math

import jax
import jax.numpy as jnp
from jax import lax
from jax.experimental import pallas as pl
from jax.experimental.pallas import tpu as pltpu
from jax.sharding import PartitionSpec as P

HEAD_DIM = 64
LANES = 2 * HEAD_DIM
SPAN = 8
MESH = pl.DeviceIdType.MESH

epsilon = 1e-06
ANY = pl.BlockSpec(memory_space=pl.ANY)
VMEM = pl.BlockSpec(memory_space=pltpu.VMEM)


def meet(axis, n):
    me = lax.axis_index(axis)
    barrier = pltpu.get_barrier_semaphore()
    for k in range(1, n):
        pl.semaphore_signal(
            barrier, inc=1, device_id={axis: lax.rem(me + k, n)}, device_id_type=MESH
        )
    pl.semaphore_wait(barrier, n - 1)


def remote(src, dst, send, recv, axis, peer):
    return pltpu.make_async_remote_copy(
        src_ref=src,
        dst_ref=dst,
        send_sem=send,
        recv_sem=recv,
        device_id={axis: peer},
        device_id_type=MESH,
    )


def part(ref, dim, index, size):
    window = pl.ds(pl.multiple_of(index * size, size), size)
    return ref.at[:, window] if dim == 1 else ref.at[window, :]


def gather_kernel(axis, n, dim, size, x_ref, o_ref, send, recv, local):
    me = lax.axis_index(axis)
    meet(axis, n)
    slot = part(o_ref, dim, me, size)
    copies = []
    for k in range(1, n):
        copy = remote(x_ref, slot, send.at[k - 1], recv.at[k - 1], axis, lax.rem(me + k, n))
        copy.start()
        copies.append(copy)
    own = pltpu.make_async_copy(x_ref, slot, local)
    own.start()
    own.wait()
    for copy in copies:
        copy.wait()


def split_kernel(axis, n, dim, size, x_ref, o_ref, send, recv, local):
    me = lax.axis_index(axis)
    meet(axis, n)
    copies = []
    for k in range(1, n):
        peer = lax.rem(me + k, n)
        copy = remote(
            part(x_ref, dim, peer, size),
            o_ref.at[me],
            send.at[k - 1],
            recv.at[k - 1],
            axis,
            peer,
        )
        copy.start()
        copies.append(copy)
    own = pltpu.make_async_copy(part(x_ref, dim, me, size), o_ref.at[me], local)
    own.start()
    own.wait()
    for copy in copies:
        copy.wait()


def comm_call(kernel, out, n, identity, x):
    return pl.pallas_call(
        kernel,
        out_shape=out,
        in_specs=[ANY],
        out_specs=ANY,
        scratch_shapes=[
            pltpu.SemaphoreType.DMA((n - 1,)),
            pltpu.SemaphoreType.DMA((n - 1,)),
            pltpu.SemaphoreType.DMA,
        ],
        compiler_params=pltpu.CompilerParams(collective_id=identity, has_side_effects=True),
    )(x)


def gather(x, axis, dim, identity):
    n = lax.axis_size(axis)
    shape = list(x.shape)
    shape[dim] *= n
    kernel = functools.partial(gather_kernel, axis, n, dim, x.shape[dim])
    return comm_call(kernel, jax.ShapeDtypeStruct(tuple(shape), x.dtype), n, identity, x)


def scatter_sum(x, axis, dim, identity):
    n = lax.axis_size(axis)
    shape = list(x.shape)
    shape[dim] //= n
    kernel = functools.partial(split_kernel, axis, n, dim, shape[dim])
    parts = comm_call(kernel, jax.ShapeDtypeStruct((n, *shape), x.dtype), n, identity, x)
    return jnp.sum(parts.astype(jnp.float32), axis=0)


def memory_kernel(
    n, grads_ref, first_ref, forget_ref, momentum_ref, rate_ref, o_ref,
    came, stage, send, recv, send_back, recv_back, local, local_back,
):
    me = lax.axis_index("seq")
    meet("seq", n)
    copies = []
    for k in range(1, n):
        peer = lax.rem(me + k, n)
        copy = remote(
            grads_ref.at[peer], came.at[me], send.at[k - 1], recv.at[k - 1], "seq", peer
        )
        copy.start()
        copies.append(copy)
    own = pltpu.make_async_copy(grads_ref.at[me], came.at[me], local)
    own.start()
    own.wait()
    for copy in copies:
        copy.wait()

    def columns(c, carry):
        window = pl.ds(pl.multiple_of(c * 128, 128), 128)
        weight = first_ref[:, window]
        speed = jnp.zeros_like(weight)
        for g in range(n):
            stage[g, :, window] = weight.astype(jnp.bfloat16)
            if g < n - 1:
                grad = came[g, :, window].astype(jnp.float32)
                speed = momentum_ref[g] * speed - rate_ref[g] * grad
                weight = (1.0 - forget_ref[g]) * weight + speed
        return carry

    lax.fori_loop(0, first_ref.shape[1] // 128, columns, 0)

    copies = []
    for k in range(1, n):
        peer = lax.rem(me + k, n)
        copy = remote(
            stage.at[peer], o_ref.at[me], send_back.at[k - 1], recv_back.at[k - 1], "seq", peer
        )
        copy.start()
        copies.append(copy)
    own = pltpu.make_async_copy(stage.at[me], o_ref.at[me], local_back)
    own.start()
    own.wait()
    for copy in copies:
        copy.wait()


def evolve(grads, first, forget, momentum, rate, identity):
    n = grads.shape[0]
    return pl.pallas_call(
        functools.partial(memory_kernel, n),
        out_shape=jax.ShapeDtypeStruct(grads.shape, jnp.bfloat16),
        in_specs=[ANY, VMEM, VMEM, VMEM, VMEM],
        out_specs=ANY,
        scratch_shapes=[
            pltpu.VMEM(grads.shape, jnp.bfloat16),
            pltpu.VMEM(grads.shape, jnp.bfloat16),
            pltpu.SemaphoreType.DMA((n - 1,)),
            pltpu.SemaphoreType.DMA((n - 1,)),
            pltpu.SemaphoreType.DMA((n - 1,)),
            pltpu.SemaphoreType.DMA((n - 1,)),
            pltpu.SemaphoreType.DMA,
            pltpu.SemaphoreType.DMA,
        ],
        compiler_params=pltpu.CompilerParams(collective_id=identity, has_side_effects=True),
    )(grads, first, forget, momentum, rate)


def attention_kernel(
    n, heads, q_ref, kv_ref, o_ref,
    q_all, kv_all, ctx, q_send, q_recv, kv_send, kv_recv, ctx_send, ctx_recv, local,
):
    me = lax.axis_index("seq")
    chunk = me // heads
    head = lax.rem(me, heads)
    other = lax.rem(me + 1, n)
    rows = q_ref.shape[0]
    slots = SPAN + heads
    first_block = chunk * heads - SPAN
    my_slot = me - first_block
    my_tile = lax.rem(me, heads)

    def lanes(ref, which):
        return ref.at[:, pl.ds(pl.multiple_of(which * LANES, LANES), LANES)]

    def outgoing(k):
        peer = lax.rem(me + k, n)
        peer_chunk = peer // heads
        peer_head = lax.rem(peer, heads)
        slot = me - peer_chunk * heads + SPAN
        wanted = jnp.logical_and(slot >= 0, slot < slots)
        same = peer_chunk == chunk
        safe = jnp.where(wanted, slot, 0)
        kv_copy = remote(
            lanes(kv_ref, peer_head), kv_all.at[safe], kv_send.at[k - 1], kv_recv.at[safe], "seq", peer
        )
        q_copy = remote(
            lanes(q_ref, peer_head), q_all.at[my_tile], q_send.at[k - 1], q_recv.at[my_tile], "seq", peer
        )
        return wanted, same, kv_copy, q_copy

    meet("seq", n)
    own_kv = pltpu.make_async_copy(lanes(kv_ref, head), kv_all.at[my_slot], local.at[0])
    own_q = pltpu.make_async_copy(lanes(q_ref, head), q_all.at[my_tile], local.at[1])
    own_kv.start()
    own_q.start()
    for k in range(1, n):
        wanted, same, kv_copy, q_copy = outgoing(k)

        @pl.when(same)
        def _():
            q_copy.start()

        @pl.when(wanted)
        def _():
            kv_copy.start()

    own_kv.wait()
    own_q.wait()

    def await_kv(slot):
        block = first_block + slot

        @pl.when(jnp.logical_and(block >= 0, block != me))
        def _():
            remote(
                kv_all.at[slot], kv_all.at[slot], kv_send.at[0], kv_recv.at[slot], "seq", other
            ).wait_recv()

    for slot in range(SPAN):
        await_kv(slot)

    row = lax.broadcasted_iota(jnp.int32, (rows, rows), 0)
    column = lax.broadcasted_iota(jnp.int32, (rows, rows), 1)
    scale = math.log2(math.e) * HEAD_DIM**-0.5

    def scored(query, slot):
        pair = kv_all[slot]
        scores = lax.dot_general(
            query, pair, (((1,), (1,)), ((), ())), preferred_element_type=jnp.float32
        ) * scale
        lane = lax.broadcasted_iota(jnp.int32, pair.shape, 1)
        values = jnp.where(lane < HEAD_DIM, jnp.ones_like(pair), pair)
        return scores, values

    def absorb(state, scores, values):
        peak, total = state
        new_peak = jnp.maximum(peak, jnp.max(scores, axis=1, keepdims=True))
        weights = jnp.exp2(scores - new_peak).astype(jnp.bfloat16)
        total = total * jnp.exp2(peak - new_peak) + jnp.dot(
            weights, values, preferred_element_type=jnp.float32
        )
        return new_peak, total

    def returned(tile):
        return remote(
            ctx.at[tile], lanes(o_ref, head), ctx_send.at[tile], ctx_recv.at[head], "seq",
            chunk * heads + tile,
        )

    def one_tile(tile, carry):
        @pl.when(tile != my_tile)
        def _():
            remote(
                q_all.at[tile], q_all.at[tile], q_send.at[0], q_recv.at[tile], "seq", other
            ).wait_recv()

        await_kv(tile + SPAN)
        query = q_all[tile]
        block = chunk * heads + tile
        scores, values = scored(query, tile + SPAN)
        scores = jnp.where(column <= row, scores, -1e30)
        peak = jnp.max(scores, axis=1, keepdims=True)
        weights = jnp.exp2(scores - peak).astype(jnp.bfloat16)
        state = (peak, jnp.dot(weights, values, preferred_element_type=jnp.float32))

        def whole(back, state):
            scores, values = scored(query, tile + SPAN - back)
            return absorb(state, scores, values)

        state = lax.fori_loop(1, jnp.minimum(block, SPAN - 1) + 1, whole, state)

        def oldest(back, state):
            scores, values = scored(query, tile)
            return absorb(state, jnp.where(column > row, scores, -1e30), values)

        peak, total = lax.fori_loop(0, jnp.where(block >= SPAN, 1, 0), oldest, state)
        ctx[tile] = (total / total[:, :1]).astype(jnp.bfloat16)

        @pl.when(tile != my_tile)
        def _():
            returned(tile).start()

        @pl.when(tile == my_tile)
        def _():
            pltpu.make_async_copy(ctx.at[tile], lanes(o_ref, head), local.at[2]).start()

        return carry

    lax.fori_loop(0, heads, one_tile, 0)

    pltpu.make_async_copy(ctx.at[my_tile], lanes(o_ref, head), local.at[2]).wait()
    for tile in range(heads):
        @pl.when(tile != my_tile)
        def _():
            returned(tile).wait_send()
            remote(
                ctx.at[tile], lanes(o_ref, tile), ctx_send.at[tile], ctx_recv.at[tile], "seq", other
            ).wait_recv()

    for k in range(1, n):
        wanted, same, kv_copy, q_copy = outgoing(k)

        @pl.when(same)
        def _():
            q_copy.wait_send()

        @pl.when(wanted)
        def _():
            kv_copy.wait_send()


def attend(query, pairs, identity):
    n = lax.axis_size("seq")
    rows = query.shape[0]
    heads = query.shape[1] // LANES
    return pl.pallas_call(
        functools.partial(attention_kernel, n, heads),
        out_shape=jax.ShapeDtypeStruct(query.shape, jnp.bfloat16),
        in_specs=[ANY, ANY],
        out_specs=ANY,
        scratch_shapes=[
            pltpu.VMEM((heads, rows, LANES), jnp.bfloat16),
            pltpu.VMEM((SPAN + heads, rows, LANES), jnp.bfloat16),
            pltpu.VMEM((heads, rows, LANES), jnp.bfloat16),
            pltpu.SemaphoreType.DMA((n - 1,)),
            pltpu.SemaphoreType.DMA((heads,)),
            pltpu.SemaphoreType.DMA((n - 1,)),
            pltpu.SemaphoreType.DMA((SPAN + heads,)),
            pltpu.SemaphoreType.DMA((heads,)),
            pltpu.SemaphoreType.DMA((heads,)),
            pltpu.SemaphoreType.DMA((3,)),
        ],
        compiler_params=pltpu.CompilerParams(collective_id=identity, has_side_effects=True),
    )(query, pairs)


def silu_slope(values):
    sigmoid = jax.nn.sigmoid(values)
    return sigmoid * (1.0 + values * (1.0 - sigmoid))


def contract(left, right, left_dim, right_dim):
    return lax.dot_general(
        left,
        right,
        (((left_dim,), (right_dim,)), ((), ())),
        preferred_element_type=jnp.float32,
    )


def normalize(retrieved, norm_gain):
    mean_square = jnp.mean(retrieved * retrieved, axis=-1, keepdims=True)
    return (retrieved * lax.rsqrt(mean_square + epsilon) * norm_gain).astype(jnp.bfloat16)


def narrow(x):
    return x.astype(jnp.bfloat16)


def paired(left, right):
    depth, width = right.shape
    left, right = (a.reshape(depth, width // HEAD_DIM, HEAD_DIM) for a in (left, right))
    return jnp.concatenate([left, right], axis=2).reshape(depth, 2 * width)


def shards(
    tokens,
    mem_query_w,
    mem_key_w,
    mem_value_w,
    mem_in,
    mem_out,
    forget_levels,
    momentum_levels,
    step_levels,
    plan,
    norm_gain,
    attn_query_w,
    attn_key_w,
    attn_value_w,
    attn_out_w,
):
    tok_rows, width = tokens.shape
    n_seq = lax.axis_size("seq")
    my_seq = lax.axis_index("seq")
    hidden_units = mem_out.shape[0]
    share = hidden_units // n_seq
    key_part = narrow(contract(tokens, mem_key_w, 1, 0))
    mem_key = gather(key_part, "head", 1, 0)
    mem_query = lax.all_gather(
        narrow(contract(tokens, mem_query_w, 1, 0)), "head", axis=1, tiled=True
    )
    value_part = narrow(contract(tokens, mem_value_w, 1, 0)).astype(jnp.float32)
    plan_all = lax.all_gather(plan, "seq", axis=0, tiled=True)

    in_turned = mem_in.T
    out_narrow = narrow(mem_out)
    pre_act = contract(mem_key, narrow(mem_in), 1, 0)
    hidden = narrow(jax.nn.silu(pre_act))
    predicted = scatter_sum(narrow(contract(hidden, out_narrow, 1, 0)), "head", 1, 1)
    residual_err = gather(narrow(2.0 / tok_rows * (predicted - value_part)), "head", 1, 2)
    grad_out = contract(hidden, residual_err, 0, 0)
    slope_term = narrow(contract(residual_err, out_narrow, 1, 1) * silu_slope(pre_act))
    grad_in = contract(slope_term, mem_key, 0, 0)
    grads = narrow(jnp.concatenate([grad_in, grad_out], axis=1)).reshape(
        n_seq, share, 2 * width
    )

    def mine(array, dim):
        return lax.dynamic_slice_in_dim(array, my_seq * share, share, dim)

    first = jnp.concatenate([mine(in_turned, 0), mine(mem_out, 0)], axis=1)
    matches = plan_all[:, None] == jnp.arange(forget_levels.shape[0], dtype=jnp.int32)[None, :]

    def gate(table):
        chosen = jnp.sum(jnp.where(matches[:, :, None], mine(table, 1)[None], 0.0), axis=1)
        return jnp.broadcast_to(chosen[:, :, None], (n_seq, share, 128))

    weights = evolve(
        grads, first, gate(forget_levels), gate(momentum_levels), gate(step_levels), 3
    ).reshape(hidden_units, 2 * width)
    query_hidden = narrow(jax.nn.silu(contract(mem_query, weights[:, :width], 1, 1)))
    retrieved = scatter_sum(
        narrow(contract(query_hidden, weights[:, width:], 1, 0)), "head", 0, 4
    )
    normed = gather(normalize(retrieved, norm_gain), "head", 0, 5)
    query_w = paired(attn_query_w, jnp.zeros_like(attn_query_w))
    pair_w = paired(attn_key_w, attn_value_w)
    att_query = narrow(contract(normed, query_w, 1, 0))
    att_pairs = narrow(contract(normed, pair_w, 1, 0))
    context = attend(att_query, att_pairs, 6)
    heads = attn_out_w.shape[0] // HEAD_DIM
    out_rows = attn_out_w.reshape(heads, HEAD_DIM, width)
    out_w = jnp.concatenate([jnp.zeros_like(out_rows), out_rows], axis=1).reshape(
        heads * LANES, width
    )
    return narrow(scatter_sum(narrow(contract(context, out_w, 1, 0)), "head", 1, 7))


def solution(mesh):
    in_specs = (
        P("seq", None),
        P(None, "head"),
        P(None, "head"),
        P(None, "head"),
        P(None, "head"),
        P("head", None),
        P(None, "head"),
        P(None, "head"),
        P(None, "head"),
        P("seq"),
        P(),
        P(None, "head"),
        P(None, "head"),
        P(None, "head"),
        P("head", None),
    )
    out_specs = P("seq", "head")
    return jax.shard_map(shards, mesh=mesh, in_specs=in_specs, out_specs=out_specs, check_vma=False)
```

```python
import functools
import math

import jax
import jax.numpy as jnp
from jax import lax
from jax.experimental import pallas as pl
from jax.experimental.pallas import tpu as pltpu
from jax.sharding import PartitionSpec as P

HEAD_DIM = 64
LANES = 2 * HEAD_DIM
SPAN = 8
MESH = pl.DeviceIdType.MESH

epsilon = 1e-06
ANY = pl.BlockSpec(memory_space=pl.ANY)
VMEM = pl.BlockSpec(memory_space=pltpu.VMEM)


def meet(axis, n):
    me = lax.axis_index(axis)
    barrier = pltpu.get_barrier_semaphore()
    for k in range(1, n):
        pl.semaphore_signal(
            barrier, inc=1, device_id={axis: lax.rem(me + k, n)}, device_id_type=MESH
        )
    pl.semaphore_wait(barrier, n - 1)


def remote(src, dst, send, recv, axis, peer):
    return pltpu.make_async_remote_copy(
        src_ref=src,
        dst_ref=dst,
        send_sem=send,
        recv_sem=recv,
        device_id={axis: peer},
        device_id_type=MESH,
    )


def part(ref, dim, index, size):
    window = pl.ds(pl.multiple_of(index * size, size), size)
    return ref.at[:, window] if dim == 1 else ref.at[window, :]


def gather_kernel(axis, n, dim, size, x_ref, o_ref, send, recv, local):
    me = lax.axis_index(axis)
    meet(axis, n)
    slot = part(o_ref, dim, me, size)
    copies = []
    for k in range(1, n):
        copy = remote(x_ref, slot, send.at[k - 1], recv.at[k - 1], axis, lax.rem(me + k, n))
        copy.start()
        copies.append(copy)
    own = pltpu.make_async_copy(x_ref, slot, local)
    own.start()
    own.wait()
    for copy in copies:
        copy.wait()


def split_kernel(axis, n, dim, size, x_ref, o_ref, send, recv, local):
    me = lax.axis_index(axis)
    meet(axis, n)
    copies = []
    for k in range(1, n):
        peer = lax.rem(me + k, n)
        copy = remote(
            part(x_ref, dim, peer, size),
            o_ref.at[me],
            send.at[k - 1],
            recv.at[k - 1],
            axis,
            peer,
        )
        copy.start()
        copies.append(copy)
    own = pltpu.make_async_copy(part(x_ref, dim, me, size), o_ref.at[me], local)
    own.start()
    own.wait()
    for copy in copies:
        copy.wait()


def comm_call(kernel, out, n, identity, x):
    return pl.pallas_call(
        kernel,
        out_shape=out,
        in_specs=[ANY],
        out_specs=ANY,
        scratch_shapes=[
            pltpu.SemaphoreType.DMA((n - 1,)),
            pltpu.SemaphoreType.DMA((n - 1,)),
            pltpu.SemaphoreType.DMA,
        ],
        compiler_params=pltpu.CompilerParams(collective_id=identity, has_side_effects=True),
    )(x)


def gather(x, axis, dim, identity):
    n = lax.axis_size(axis)
    shape = list(x.shape)
    shape[dim] *= n
    kernel = functools.partial(gather_kernel, axis, n, dim, x.shape[dim])
    return comm_call(kernel, jax.ShapeDtypeStruct(tuple(shape), x.dtype), n, identity, x)


def scatter_sum(x, axis, dim, identity):
    n = lax.axis_size(axis)
    shape = list(x.shape)
    shape[dim] //= n
    kernel = functools.partial(split_kernel, axis, n, dim, shape[dim])
    parts = comm_call(kernel, jax.ShapeDtypeStruct((n, *shape), x.dtype), n, identity, x)
    return jnp.sum(parts.astype(jnp.float32), axis=0)


def whole_sum(x, axis, identity):
    parts = gather(x, axis, 0, identity).reshape(-1, *x.shape)
    return jnp.sum(parts.astype(jnp.float32), axis=0)


def memory_kernel(
    n, grads_ref, gates_ref, first_ref, o_ref,
    came, gates, wide, stage, send, recv, send_gate, recv_gate, send_back, recv_back, local,
):
    me = lax.axis_index("seq")
    meet("seq", n)
    copies = []
    for k in range(1, n):
        peer = lax.rem(me + k, n)
        gate_copy = remote(
            gates_ref.at[peer], gates.at[me], send_gate.at[k - 1], recv_gate.at[k - 1], "seq", peer
        )
        gate_copy.start()
        copy = remote(
            grads_ref.at[peer], came.at[me], send.at[k - 1], recv.at[k - 1], "seq", peer
        )
        copy.start()
        copies += [gate_copy, copy]
    own_gates = pltpu.make_async_copy(gates_ref.at[me], gates.at[me], local.at[0])
    own_gates.start()
    own = pltpu.make_async_copy(grads_ref.at[me], came.at[me], local.at[1])
    own.start()
    own_gates.wait()
    own.wait()
    for copy in copies:
        copy.wait()

    for g in range(n):
        row = gates[g]
        for which in range(3):
            wide[which, g] = jnp.broadcast_to(row[:, which : which + 1], row.shape)

    def columns(c, carry):
        window = pl.ds(pl.multiple_of(c * 128, 128), 128)
        weight = first_ref[:, window]
        speed = jnp.zeros_like(weight)
        for g in range(n):
            stage[g, :, window] = weight.astype(jnp.bfloat16)
            if g < n - 1:
                grad = came[g, :, window].astype(jnp.float32)
                speed = wide[0, g] * speed - wide[2, g] * grad
                weight = (1.0 - wide[1, g]) * weight + speed
        return carry

    lax.fori_loop(0, first_ref.shape[1] // 128, columns, 0)

    copies = []
    for k in range(1, n):
        peer = lax.rem(me + k, n)
        copy = remote(
            stage.at[peer], o_ref.at[me], send_back.at[k - 1], recv_back.at[k - 1], "seq", peer
        )
        copy.start()
        copies.append(copy)
    own = pltpu.make_async_copy(stage.at[me], o_ref.at[me], local.at[2])
    own.start()
    own.wait()
    for copy in copies:
        copy.wait()


def evolve(grads, gates, first, identity):
    n = grads.shape[0]
    return pl.pallas_call(
        functools.partial(memory_kernel, n),
        out_shape=jax.ShapeDtypeStruct(grads.shape, jnp.bfloat16),
        in_specs=[ANY, ANY, VMEM],
        out_specs=ANY,
        scratch_shapes=[
            pltpu.VMEM(grads.shape, jnp.bfloat16),
            pltpu.VMEM(gates.shape, jnp.float32),
            pltpu.VMEM((3, *gates.shape), jnp.float32),
            pltpu.VMEM(grads.shape, jnp.bfloat16),
            *[pltpu.SemaphoreType.DMA((n - 1,))] * 6,
            pltpu.SemaphoreType.DMA((3,)),
        ],
        compiler_params=pltpu.CompilerParams(collective_id=identity, has_side_effects=True),
    )(grads, gates, first)


def attention_kernel(
    n, heads, q_ref, kv_ref, o_ref,
    q_all, kv_all, ctx, peaks, totals, q_send, q_recv, kv_send, kv_recv, ctx_send, ctx_recv, local,
):
    me = lax.axis_index("seq")
    chunk = me // heads
    head = lax.rem(me, heads)
    other = lax.rem(me + 1, n)
    rows = q_ref.shape[0]
    slots = SPAN + heads
    first_block = chunk * heads - SPAN
    my_slot = me - first_block
    my_tile = lax.rem(me, heads)

    def lanes(ref, which):
        return ref.at[:, pl.ds(pl.multiple_of(which * LANES, LANES), LANES)]

    def outgoing(k):
        peer = lax.rem(me + k, n)
        peer_chunk = peer // heads
        peer_head = lax.rem(peer, heads)
        slot = me - peer_chunk * heads + SPAN
        wanted = jnp.logical_and(slot >= 0, slot < slots)
        same = peer_chunk == chunk
        safe = jnp.where(wanted, slot, 0)
        kv_copy = remote(
            lanes(kv_ref, peer_head), kv_all.at[safe], kv_send.at[k - 1], kv_recv.at[safe], "seq", peer
        )
        q_copy = remote(
            lanes(q_ref, peer_head), q_all.at[my_tile], q_send.at[k - 1], q_recv.at[my_tile], "seq", peer
        )
        return wanted, same, kv_copy, q_copy

    meet("seq", n)
    own_kv = pltpu.make_async_copy(lanes(kv_ref, head), kv_all.at[my_slot], local.at[0])
    own_q = pltpu.make_async_copy(lanes(q_ref, head), q_all.at[my_tile], local.at[1])
    own_kv.start()
    own_q.start()
    for k in range(1, n):
        wanted, same, kv_copy, q_copy = outgoing(k)

        @pl.when(same)
        def _():
            q_copy.start()

        @pl.when(wanted)
        def _():
            kv_copy.start()

    own_kv.wait()
    own_q.wait()

    def await_kv(slot):
        block = first_block + slot

        @pl.when(jnp.logical_and(block >= 0, block != me))
        def _():
            remote(
                kv_all.at[slot], kv_all.at[slot], kv_send.at[0], kv_recv.at[slot], "seq", other
            ).wait_recv()

    row = lax.broadcasted_iota(jnp.int32, (rows, rows), 0)
    column = lax.broadcasted_iota(jnp.int32, (rows, rows), 1)
    scale = math.log2(math.e) * HEAD_DIM**-0.5

    def scored(query, slot):
        pair = kv_all[slot]
        scores = lax.dot_general(
            query, pair, (((1,), (1,)), ((), ())), preferred_element_type=jnp.float32
        ) * scale
        lane = lax.broadcasted_iota(jnp.int32, pair.shape, 1)
        values = jnp.where(lane < HEAD_DIM, jnp.ones_like(pair), pair)
        return scores, values

    def absorb(state, scores, values):
        peak, total = state
        new_peak = jnp.maximum(peak, jnp.max(scores, axis=1, keepdims=True))
        weights = jnp.exp2(scores - new_peak).astype(jnp.bfloat16)
        total = total * jnp.exp2(peak - new_peak) + jnp.dot(
            weights, values, preferred_element_type=jnp.float32
        )
        return new_peak, total

    def returned(tile):
        return remote(
            ctx.at[tile], lanes(o_ref, head), ctx_send.at[tile], ctx_recv.at[head], "seq",
            chunk * heads + tile,
        )

    def near(tile, carry):
        @pl.when(tile != my_tile)
        def _():
            remote(
                q_all.at[tile], q_all.at[tile], q_send.at[0], q_recv.at[tile], "seq", other
            ).wait_recv()

        await_kv(tile + SPAN)
        query = q_all[tile]
        scores, values = scored(query, tile + SPAN)
        scores = jnp.where(column <= row, scores, -1e30)
        peak = jnp.max(scores, axis=1, keepdims=True)
        weights = jnp.exp2(scores - peak).astype(jnp.bfloat16)
        state = (peak, jnp.dot(weights, values, preferred_element_type=jnp.float32))

        def whole(back, state):
            scores, values = scored(query, tile + SPAN - back)
            return absorb(state, scores, values)

        peak, total = lax.fori_loop(1, jnp.minimum(tile, SPAN - 1) + 1, whole, state)
        peaks[tile] = peak
        totals[tile] = total
        return carry

    def far(step, carry):
        tile = heads - 1 - step
        block = chunk * heads + tile

        @pl.when(tile < SPAN)
        def _():
            await_kv(tile)

        query = q_all[tile]

        def whole(back, state):
            scores, values = scored(query, tile + SPAN - back)
            return absorb(state, scores, values)

        state = lax.fori_loop(
            jnp.minimum(tile, SPAN - 1) + 1,
            jnp.minimum(block, SPAN - 1) + 1,
            whole,
            (peaks[tile], totals[tile]),
        )

        def oldest(back, state):
            scores, values = scored(query, tile)
            return absorb(state, jnp.where(column > row, scores, -1e30), values)

        peak, total = lax.fori_loop(0, jnp.where(block >= SPAN, 1, 0), oldest, state)
        ctx[tile] = (total / total[:, :1]).astype(jnp.bfloat16)

        @pl.when(tile != my_tile)
        def _():
            returned(tile).start()

        @pl.when(tile == my_tile)
        def _():
            pltpu.make_async_copy(ctx.at[tile], lanes(o_ref, head), local.at[2]).start()

        return carry

    lax.fori_loop(0, heads, near, 0)
    for slot in range(heads, SPAN):
        await_kv(slot)
    lax.fori_loop(0, heads, far, 0)

    pltpu.make_async_copy(ctx.at[my_tile], lanes(o_ref, head), local.at[2]).wait()
    for tile in range(heads):
        @pl.when(tile != my_tile)
        def _():
            returned(tile).wait_send()
            remote(
                ctx.at[tile], lanes(o_ref, tile), ctx_send.at[tile], ctx_recv.at[tile], "seq", other
            ).wait_recv()

    for k in range(1, n):
        wanted, same, kv_copy, q_copy = outgoing(k)

        @pl.when(same)
        def _():
            q_copy.wait_send()

        @pl.when(wanted)
        def _():
            kv_copy.wait_send()


def attend(query, pairs, identity):
    n = lax.axis_size("seq")
    rows = query.shape[0]
    heads = query.shape[1] // LANES
    return pl.pallas_call(
        functools.partial(attention_kernel, n, heads),
        out_shape=jax.ShapeDtypeStruct(query.shape, jnp.bfloat16),
        in_specs=[ANY, ANY],
        out_specs=ANY,
        scratch_shapes=[
            pltpu.VMEM((heads, rows, LANES), jnp.bfloat16),
            pltpu.VMEM((SPAN + heads, rows, LANES), jnp.bfloat16),
            pltpu.VMEM((heads, rows, LANES), jnp.bfloat16),
            pltpu.VMEM((heads, rows, 1), jnp.float32),
            pltpu.VMEM((heads, rows, LANES), jnp.float32),
            pltpu.SemaphoreType.DMA((n - 1,)),
            pltpu.SemaphoreType.DMA((heads,)),
            pltpu.SemaphoreType.DMA((n - 1,)),
            pltpu.SemaphoreType.DMA((SPAN + heads,)),
            pltpu.SemaphoreType.DMA((heads,)),
            pltpu.SemaphoreType.DMA((heads,)),
            pltpu.SemaphoreType.DMA((3,)),
        ],
        compiler_params=pltpu.CompilerParams(collective_id=identity, has_side_effects=True),
    )(query, pairs)


def silu_slope(values):
    sigmoid = jax.nn.sigmoid(values)
    return sigmoid * (1.0 + values * (1.0 - sigmoid))


def contract(left, right, left_dim, right_dim):
    return lax.dot_general(
        left,
        right,
        (((left_dim,), (right_dim,)), ((), ())),
        preferred_element_type=jnp.float32,
    )


def normalize(retrieved, norm_gain):
    mean_square = jnp.mean(retrieved * retrieved, axis=-1, keepdims=True)
    return (retrieved * lax.rsqrt(mean_square + epsilon) * norm_gain).astype(jnp.bfloat16)


def narrow(x):
    return x.astype(jnp.bfloat16)


def paired(left, right):
    depth, width = right.shape
    left, right = (a.reshape(depth, width // HEAD_DIM, HEAD_DIM) for a in (left, right))
    return jnp.concatenate([left, right], axis=2).reshape(depth, 2 * width)


def shards(
    tokens,
    mem_query_w,
    mem_key_w,
    mem_value_w,
    mem_in,
    mem_out,
    forget_levels,
    momentum_levels,
    step_levels,
    plan,
    norm_gain,
    attn_query_w,
    attn_key_w,
    attn_value_w,
    attn_out_w,
):
    tok_rows, width = tokens.shape
    n_seq = lax.axis_size("seq")
    my_seq = lax.axis_index("seq")
    hidden_units = mem_out.shape[0]
    share = hidden_units // n_seq
    key_part = narrow(contract(tokens, mem_key_w, 1, 0))
    mem_key = gather(key_part, "head", 1, 0)
    mem_query = lax.all_gather(
        narrow(contract(tokens, mem_query_w, 1, 0)), "head", axis=1, tiled=True
    )
    value_part = narrow(contract(tokens, mem_value_w, 1, 0)).astype(jnp.float32)
    pair = lax.axis_size("head") <= 2
    out_narrow = narrow(mem_out)
    pre_act = contract(mem_key, narrow(mem_in), 1, 0)
    hidden = narrow(jax.nn.silu(pre_act))
    partial = contract(hidden, out_narrow, 1, 0)
    if pair:
        mine_first = lax.axis_index("head") * value_part.shape[1]
        value_wide = lax.dynamic_update_slice_in_dim(
            jnp.zeros_like(partial), value_part, mine_first, 1
        )
        residual_err = narrow(2.0 / tok_rows * whole_sum(narrow(partial - value_wide), "head", 1))
    else:
        predicted = scatter_sum(narrow(partial), "head", 1, 1)
        residual_err = gather(narrow(2.0 / tok_rows * (predicted - value_part)), "head", 1, 2)
    grad_out = contract(hidden, residual_err, 0, 0)
    slope_term = narrow(contract(residual_err, out_narrow, 1, 1) * silu_slope(pre_act))
    grad_in = contract(slope_term, mem_key, 0, 0)
    grads = narrow(jnp.concatenate([grad_in, grad_out], axis=1)).reshape(
        n_seq, share, 2 * width
    )

    def mine(array, dim):
        return lax.dynamic_slice_in_dim(array, my_seq * share, share, dim)

    first = jnp.concatenate([mine(mem_in, 1).T, mine(mem_out, 0)], axis=1)
    matches = jnp.arange(forget_levels.shape[0], dtype=jnp.int32)[:, None] == plan[0]
    chosen = [
        jnp.sum(jnp.where(matches, table, 0.0), axis=0)
        for table in (momentum_levels, forget_levels, step_levels)
    ]
    gates = jnp.pad(jnp.stack(chosen, axis=1), ((0, 0), (0, 125))).reshape(n_seq, share, 128)
    weights = evolve(grads, gates, first, 3).reshape(hidden_units, 2 * width)
    query_hidden = narrow(jax.nn.silu(contract(mem_query, weights[:, :width], 1, 1)))
    partial = narrow(contract(query_hidden, weights[:, width:], 1, 0))
    if pair:
        normed = normalize(whole_sum(partial, "head", 4), norm_gain)
    else:
        retrieved = scatter_sum(partial, "head", 0, 4)
        normed = gather(normalize(retrieved, norm_gain), "head", 0, 5)
    query_w = paired(attn_query_w, jnp.zeros_like(attn_query_w))
    pair_w = paired(attn_key_w, attn_value_w)
    att_query = narrow(contract(normed, query_w, 1, 0))
    att_pairs = narrow(contract(normed, pair_w, 1, 0))
    context = attend(att_query, att_pairs, 6)
    heads = attn_out_w.shape[0] // HEAD_DIM
    out_rows = attn_out_w.reshape(heads, HEAD_DIM, width)
    out_w = jnp.concatenate([jnp.zeros_like(out_rows), out_rows], axis=1).reshape(
        heads * LANES, width
    )
    return narrow(scatter_sum(narrow(contract(context, out_w, 1, 0)), "head", 1, 7))


def solution(mesh):
    in_specs = (
        P("seq", None),
        P(None, "head"),
        P(None, "head"),
        P(None, "head"),
        P(None, "head"),
        P("head", None),
        P(None, "head"),
        P(None, "head"),
        P(None, "head"),
        P("seq"),
        P(),
        P(None, "head"),
        P(None, "head"),
        P(None, "head"),
        P("head", None),
    )
    out_specs = P("seq", "head")
    return jax.shard_map(shards, mesh=mesh, in_specs=in_specs, out_specs=out_specs, check_vma=False)
```
